32 devices in a mesh: seq: 16 (over z, y, x), tp: 2 (over core).
Axes of the slice: x: 2, y: 2, z: 4, core: 2. Of those that a mesh axis runs over, the one named last changes fastest.
Arguments:
- inner_input: bfloat16 [4096, 2560], P('seq', 'tp'), may hold values from -6 to 6
- gate_input: bfloat16 [4096, 2560], P('seq', 'tp'), may hold values from -170 to 170
- state_input: bfloat16 [4096, 256], P('seq'), may hold values from -6 to 6
- step_raw: float32 [40, 4096], P('tp', 'seq'), may hold values from -14 to 0
- conv_inner: float32 [4, 2560], P(None, 'tp'), may hold values from -3 to 3
- conv_state: float32 [4, 256], replicated, may hold values from -3 to 3
- bias_inner: float32 [2560], P('tp'), may hold values from -3 to 3
- bias_state: float32 [256], replicated, may hold values from -3 to 3
- step_bias: float32 [40], P('tp'), may hold values from -0.3 to 0.3
- decay_log: float32 [40], P('tp'), may hold values from -1.4 to 0
- skip_gain: float32 [40], P('tp'), may hold values from 0.5 to 1.5
- norm_gain: float32 [2560], P('tp'), may hold values from 0.1 to 1.9
- out_weight: bfloat16 [2560, 2560], P('tp'), may hold values from -0.15625 to 0.15625
Outputs:
- block_out: bfloat16 [4096, 2560], P('seq', 'tp')
The draws below stay inside these ranges and needn't reach their ends.
All inputs are finite; a program needn't handle non-finite values.
Results may differ from the reference program's by a relative error of at most 0.008.
Values may be sent and summed in bfloat16 or wider, within the bound.
A program may use at most 64 MiB of HBM per device.

```python
import math
import jax
import jax.numpy as jnp
from jax import lax

D = 2560
HEADS = 40
HEAD_DIM = 64
NSTATE = 128
KW = 4
INNER = 2560
TOKEN_COUNT = 4096


def draw_gate_input(key, part):
    second = jax.random.fold_in(key, 1)
    columns = jnp.arange(INNER, dtype=jnp.float32) / INNER
    values = jnp.clip(jax.random.normal(second, (TOKEN_COUNT, INNER)), -5.0, 5.0)
    return (values * jnp.exp(jnp.log(3.0) * columns)[None, :]).astype(jnp.bfloat16)


def draw_step_raw(key, part):
    random_keys = jax.random.split(key, 4)
    share = 0.5
    slow_heads = jax.random.uniform(random_keys[0], (HEADS,)) < share
    base_step = jnp.exp(jax.random.uniform(random_keys[1], (HEADS,), minval=jnp.log(0.05), maxval=jnp.log(0.2)))
    jitter_amount = jnp.exp(jax.random.uniform(random_keys[2], (HEADS, TOKEN_COUNT), minval=-0.7, maxval=0.7))
    spike_points = jax.random.randint(random_keys[3], (4,), 0, TOKEN_COUNT)
    at_spike_point = jnp.any(jnp.arange(TOKEN_COUNT)[None, :] == spike_points[:, None], axis=0)
    gentle_step = jnp.where(at_spike_point[None, :], 0.25, jitter_amount / TOKEN_COUNT)
    target = jnp.where(slow_heads[:, None], gentle_step, base_step[:, None] * jitter_amount)
    return jnp.log(jnp.expm1(target)).astype(jnp.float32)


def with_spikes(result, key, source, target, shards_of, factor):
    owner, partner = [(jnp.arange(result.shape[dim]) // (result.shape[dim] // shards_of)).reshape([-1 if axis == dim else 1 for axis in range(result.ndim)]) for dim in (source, target)]
    chosen = jax.random.permutation(key, shards_of)[partner]
    strong = (owner == chosen) | (owner == (partner + shards_of // 2) % shards_of)
    return jnp.where(strong, factor * result, result)


def block_levels(stream_key, dims, cuts, low, largest):
    loudness, own = 1.0, jax.random.fold_in(stream_key, 6)
    for dim, parts in cuts:
        draws = jnp.exp(jax.random.uniform(jax.random.fold_in(own, dim), (parts,), jnp.float32, low / len(cuts), largest / len(cuts)))
        loudness = loudness * jnp.repeat(draws, dims[dim] // parts).reshape([-1 if axis == dim else 1 for axis in range(len(dims))])
    return loudness


def scatter_about(stream_key, shape, scale, most, shards=(), kind=jnp.bfloat16):
    array = jax.random.normal(stream_key, shape, jnp.float32) * scale
    if len(shards) > 0:
        array = block_levels(stream_key, shape, shards, -0.22, 0.18) * array
    return jnp.clip(array, min=-most, max=most).astype(kind)


def heavy_noise(stream_key, shape, width, most, cuts, heavy, kind=jnp.bfloat16):
    array = width * jax.random.normal(stream_key, shape, jnp.float32)
    if cuts:
        array = array * block_levels(stream_key, shape, cuts, -0.22, 0.18)
    return jnp.clip(with_spikes(array, jax.random.fold_in(stream_key, 3), *heavy), -most, most).astype(kind)


def setup_inputs(seed: int = 0) -> dict:
    seeds = jax.random.split(jax.random.key(seed), 14)
    return {
        "inner_input": scatter_about(seeds[0], (TOKEN_COUNT, INNER), 1.0, 6.0, ((0, 16), (1, 2))),
        "gate_input": draw_gate_input(jax.random.fold_in(seeds[13], 71), 0),
        "state_input": scatter_about(seeds[2], (TOKEN_COUNT, 2 * NSTATE), 1.0, 6.0, ((0, 16),)),
        "step_raw": draw_step_raw(jax.random.fold_in(seeds[13], 71), 0),
        "conv_inner": scatter_about(seeds[4], (KW, INNER), KW ** -0.5, 3.0, ((1, 2),), jnp.float32),
        "conv_state": scatter_about(seeds[5], (KW, 2 * NSTATE), KW ** -0.5, 3.0, (), jnp.float32),
        "bias_inner": scatter_about(seeds[6], (INNER,), 0.5, 3.0, ((0, 2),), jnp.float32),
        "bias_state": scatter_about(seeds[7], (2 * NSTATE,), 0.5, 3.0, (), jnp.float32),
        "step_bias": jnp.clip(jax.random.uniform(seeds[8], (HEADS,), jnp.float32, -0.3, 0.3) * block_levels(seeds[8], (HEADS,), ((0, 2),), -0.4, 0.0), -0.3, 0.3),
        "decay_log": jnp.clip(-1.4 + 1.4 * jax.random.uniform(seeds[9], (HEADS,), jnp.float32) ** block_levels(seeds[9], (HEADS,), ((0, 2),), -0.2, 0.2), -1.4, 0.0),
        "skip_gain": jnp.clip(0.5 + 1.0 * jax.random.uniform(seeds[10], (HEADS,), jnp.float32) ** block_levels(seeds[10], (HEADS,), ((0, 2),), -0.2, 0.2), 0.5, 1.5),
        "norm_gain": jnp.clip(1.0 + 0.18 * jax.random.normal(seeds[11], (INNER,), jnp.float32), 0.1, 1.9),
        "out_weight": heavy_noise(seeds[12], (INNER, D), INNER ** -0.5, 0.15625, ((0, 2),), (0, 1, 2, 2.0)),
    }


highest = lax.Precision.HIGHEST

def conv_silu(padded, weights, offsets, length):
    width_taps = weights.shape[0]
    summed = offsets.astype(jnp.float32)[None, :] + jnp.zeros((length, weights.shape[1]), jnp.float32)
    for number in range(width_taps):
        summed = summed + weights[number][None, :] * padded[number:number + length]
    return jax.nn.silu(summed).astype(jnp.bfloat16)

def block_step(state_now, pieces):
    inner_rows, keys_b, query_c, step_sizes, log_decay = pieces
    cumulative = jnp.cumsum(log_decay, axis=1)
    block_rows = log_decay.shape[1]
    causal = jnp.arange(block_rows)[:, None] >= jnp.arange(block_rows)[None, :]
    spread = jnp.where(causal[None], cumulative[:, :, None] - cumulative[:, None, :], -jnp.inf)
    scores = jnp.dot(query_c, keys_b.T, precision=highest)
    weights = scores[None] * jnp.exp(spread) * step_sizes[:, None, :]
    output = jnp.einsum('hts,shp->thp', weights, inner_rows, precision=highest)
    carried = jnp.einsum('tn,hnp->thp', query_c, state_now, precision=highest)
    output = output + carried * jnp.exp(cumulative).T[:, :, None]
    towards_end = jnp.exp(cumulative[:, -1:] - cumulative) * step_sizes
    update = jnp.einsum('sn,shp->hnp', keys_b, inner_rows * towards_end.T[:, :, None], precision=highest)
    state_next = jnp.exp(cumulative[:, -1])[:, None, None] * state_now + update
    return (state_next, output)

def reference(inner_input, gate_input, state_input, step_raw, conv_inner, conv_state, bias_inner, bias_state, step_bias, decay_log, skip_gain, norm_gain, out_weight):
    width_taps = conv_inner.shape[0]
    pad_rows = ((width_taps - 1, 0), (0, 0))
    inner_conv = conv_silu(jnp.pad(inner_input.astype(jnp.float32), pad_rows), conv_inner, bias_inner, TOKEN_COUNT)
    state_conv = conv_silu(jnp.pad(state_input.astype(jnp.float32), pad_rows), conv_state, bias_state, TOKEN_COUNT)
    step_sizes = jax.nn.softplus(step_raw + step_bias[:, None])
    log_decay = -jnp.exp(decay_log)[:, None] * step_sizes
    block_size = math.gcd(TOKEN_COUNT, 256)
    blocks = TOKEN_COUNT // block_size
    inner_float = inner_conv.astype(jnp.float32)
    inner_rows = inner_float.reshape(blocks, block_size, HEADS, HEAD_DIM)
    keys_b = state_conv[:, :NSTATE].astype(jnp.float32).reshape(blocks, block_size, NSTATE)
    query_c = state_conv[:, NSTATE:].astype(jnp.float32).reshape(blocks, block_size, NSTATE)
    step_block_grid = step_sizes.reshape(HEADS, blocks, block_size).transpose(1, 0, 2)
    log_blocks = log_decay.reshape(HEADS, blocks, block_size).transpose(1, 0, 2)
    start_state = jnp.zeros((HEADS, NSTATE, HEAD_DIM), jnp.float32)
    final_state, outputs = lax.scan(block_step, start_state, (inner_rows, keys_b, query_c, step_block_grid, log_blocks))
    mixed = outputs.reshape(TOKEN_COUNT, HEADS, HEAD_DIM) + skip_gain[None, :, None] * inner_float.reshape(TOKEN_COUNT, HEADS, HEAD_DIM)
    gated_raw = mixed.reshape(TOKEN_COUNT, INNER) * jax.nn.silu(gate_input.astype(jnp.float32))
    squares = lax.optimization_barrier(jnp.sum(gated_raw * gated_raw, axis=1))
    scale_inv = lax.rsqrt(squares / INNER + 1e-05)
    gated = (gated_raw * norm_gain[None, :]).astype(jnp.bfloat16)
    summed = jnp.dot(gated, out_weight, preferred_element_type=jnp.float32)
    return (summed * scale_inv[:, None]).astype(jnp.bfloat16)
```

```python
import functools
import math

import jax
import jax.numpy as jnp
from jax import lax
from jax.experimental import pallas as pl
from jax.experimental.pallas import tpu as pltpu
from jax.sharding import PartitionSpec as P

HEAD_DIM = 64
NSTATE = 128
LANES = 128
GROUP = 32
RIM = 8
HEAD = 16
MESH = pl.DeviceIdType.MESH
f32 = jnp.float32
bf16 = jnp.bfloat16


def silu(v):
    return v / (1.0 + jnp.exp(-v))


def log1p_exp(v):
    u = jnp.exp(-jnp.abs(v))
    z = u / (2.0 + u)
    q = z * z
    series = jnp.full_like(q, 1.0 / 19.0)
    for odd in range(17, 0, -2):
        series = series * q + 1.0 / odd
    return jnp.maximum(v, 0.0) + 2.0 * z * series


def spread_heads(table, ones):
    high = table.astype(bf16)
    low = (table - high.astype(f32)).astype(bf16)
    out = jnp.dot(high, ones, preferred_element_type=f32)
    return out + jnp.dot(low, ones, preferred_element_type=f32)


def conv_rows(src, taps, bias, start, rows, columns):
    count = taps.shape[0]
    total = bias[...]
    for k in range(count):
        first = start + RIM - count + 1 + k
        total = total + taps[k : k + 1] * src[pl.ds(first, rows), columns]
    return silu(total)


def wait_for(ref, sem):
    pltpu.make_async_copy(ref, ref, sem).wait()


def remote(src, dst, send, recv, to):
    return pltpu.make_async_remote_copy(
        src_ref=src,
        dst_ref=dst,
        send_sem=send,
        recv_sem=recv,
        device_id=to,
        device_id_type=MESH,
    )


def split_columns(inner):
    first = -(-inner * 3 // 5 // 256) * 256
    return ((0, first), (first, inner - first))


def kernel(
    n, g,
    x_hbm, gate_hbm, state_hbm, step_hbm, taps_x_hbm, taps_s_hbm, bias_x_hbm,
    bias_s_hbm, step_bias_hbm, decay_log_hbm, skip_gain_hbm, norm_gain_hbm, w_hbm,
    out_ref,
    x_in, gate_in, state_in, step_raw, taps_x, taps_s, bias_x, bias_s,
    step_bias, decay_log, skip_gain, norm_gain, w_all,
    x_pad, s_pad, x_conv, s_conv, table, spread, cols,
    scores, mixed, gate_act, decayed, gated, main,
    rim_x, rim_s, decay_out, decay_all, decay_cols, reach,
    out0, out1, got0, got1, before0, before1, back0, back1, ent0, ent1,
    pass0, pass1, in0, in1,
    acc, part, part_got, squares, squares_got,
    load_sem, rim_send, rim_recv, d_send, d_recv, s1_send, s1_recv,
    s2_send, s2_recv, c_send, c_recv, o_send, o_recv, q_sem,
):
    me = lax.axis_index("seq")
    core = lax.axis_index("tp")
    other = 1 - core
    rows, inner = x_in.shape
    heads = step_raw.shape[0]
    tiles = inner // LANES
    per = NSTATE // g
    half = rows // 2
    mg = lax.rem(me, g)
    base = me - mg
    columns = split_columns(inner)
    part_refs = (
        (out0, got0, before0, back0, ent0, pass0, in0),
        (out1, got1, before1, back1, ent1, pass1, in1),
    )

    barrier = pltpu.get_barrier_semaphore()

    def greet(k, _):
        pl.semaphore_signal(
            barrier,
            inc=1,
            device_id={"seq": base + lax.rem(mg + k, g)},
            device_id_type=MESH,
        )
        return 0

    lax.fori_loop(1, g, greet, 0)
    pl.semaphore_signal(barrier, inc=1, device_id={"tp": other}, device_id_type=MESH)

    @pl.when(me >= g)
    def _():
        pl.semaphore_signal(
            barrier, inc=1, device_id={"seq": me - g}, device_id_type=MESH
        )

    @pl.when((me >= g) & (mg == 0))
    def _():
        pl.semaphore_signal(
            barrier, inc=1, device_id={"seq": me - 1}, device_id_type=MESH
        )

    pairs = (
        (x_hbm, x_in), (state_hbm, state_in), (step_hbm, step_raw),
        (step_bias_hbm, step_bias), (decay_log_hbm, decay_log),
        (taps_s_hbm, taps_s), (bias_s_hbm, bias_s), (taps_x_hbm, taps_x),
        (bias_x_hbm, bias_x), (skip_gain_hbm, skip_gain),
        (norm_gain_hbm, norm_gain), (gate_hbm, gate_in), (w_hbm, w_all),
    )
    loads = [
        pltpu.make_async_copy(src, dst, load_sem.at[i])
        for i, (src, dst) in enumerate(pairs)
    ]
    for load in loads:
        load.start()

    spread[...] = jnp.where(
        lax.broadcasted_iota(jnp.int32, (LANES, inner), 0) % GROUP
        == lax.broadcasted_iota(jnp.int32, (LANES, inner), 1) // HEAD_DIM,
        1.0,
        0.0,
    ).astype(bf16)
    eye = (
        lax.broadcasted_iota(jnp.int32, (heads, heads), 0)
        == lax.broadcasted_iota(jnp.int32, (heads, heads), 1)
    )

    def as_column(row):
        return jnp.sum(jnp.where(eye, row[...], 0.0), axis=1, keepdims=True)

    for load in loads[2:5]:
        load.wait()
    step = log1p_exp(step_raw[...] + as_column(step_bias))
    log_decay = -jnp.exp(as_column(decay_log)) * step
    upper = (
        lax.broadcasted_iota(jnp.int32, (rows, rows), 0)
        <= lax.broadcasted_iota(jnp.int32, (rows, rows), 1)
    ).astype(f32)
    cum = jnp.dot(
        log_decay, upper, precision=lax.Precision.HIGHEST, preferred_element_type=f32
    )
    shifted = cum - jnp.log(step)
    table[...] = jnp.zeros_like(table)
    table[0:heads] = cum
    table[GROUP : GROUP + heads] = jnp.exp(cum[:, rows - 1 : rows] - shifted)
    table[2 * GROUP : 2 * GROUP + heads] = jnp.exp(cum)
    flipped = table[...].T
    cols[...] = flipped
    lane = lax.broadcasted_iota(jnp.int32, (1, LANES), 1) // GROUP
    decay_out[...] = jnp.where(
        lane == 2, jnp.broadcast_to(flipped[rows - 1 : rows], (8, LANES)), 0.0
    )
    decay_all[mg] = decay_out[...]

    for load in (loads[0], loads[1], *loads[5:9]):
        load.wait()
    s_pad[RIM:] = state_in[...].astype(f32)
    s_conv[HEAD:] = conv_rows(
        s_pad, taps_s, bias_s, HEAD, rows - HEAD, slice(None)
    ).astype(bf16)
    for i in range(tiles):
        c = slice(i * LANES, (i + 1) * LANES)
        x_pad[RIM:, c] = x_in[:, c].astype(f32)
        x_conv[HEAD:, c] = conv_rows(
            x_pad, taps_x[:, c], bias_x[i : i + 1], HEAD, rows - HEAD, c
        ).astype(bf16)

    ahead = jnp.where(me < n - g, 1, 0)
    edge = jnp.where((mg == g - 1) & (me < n - 1), 1, 0)
    pl.semaphore_wait(barrier, g + ahead + edge)

    def rim_copies():
        target = {"seq": lax.rem(me + 1, n)}
        return [
            remote(
                src.at[pl.ds(rows - RIM, RIM)], dst, rim_send.at[i], rim_recv.at[i],
                target,
            )
            for i, (src, dst) in enumerate(((x_in, rim_x), (state_in, rim_s)))
        ]

    @pl.when(me < n - 1)
    def _():
        for copy in rim_copies():
            copy.start()

    def decay_start(k, _):
        remote(
            decay_out, decay_all.at[mg], d_send, d_recv,
            {"seq": base + lax.rem(mg + k, g)},
        ).start()
        return 0

    lax.fori_loop(1, g, decay_start, 0)

    towards = jnp.where(lane == 1, cols[...], 0.0)
    keys_main = s_conv[HEAD:, :NSTATE]
    for i in range(tiles):
        c = slice(i * LANES, (i + 1) * LANES)
        scaled = (
            x_conv[HEAD:, c].astype(f32) * spread_heads(towards[HEAD:], spread[:, c])
        ).astype(bf16)
        main[:, c] = lax.dot_general(
            keys_main, scaled, (((0,), (0,)), ((), ())), preferred_element_type=f32
        )

    loads[11].wait()
    for i in range(tiles):
        c = slice(i * LANES, (i + 1) * LANES)
        gate_act[:, c] = silu(gate_in[:, c].astype(f32))

    @pl.when(me > 0)
    def _():
        for copy in rim_copies():
            copy.wait_recv()
        s_pad[0:RIM] = rim_s[...].astype(f32)
        x_pad[0:RIM] = rim_x[...].astype(f32)

    @pl.when(me == 0)
    def _():
        s_pad[0:RIM] = jnp.zeros((RIM, s_pad.shape[1]), f32)
        x_pad[0:RIM] = jnp.zeros((RIM, inner), f32)

    s_conv[0:HEAD] = conv_rows(s_pad, taps_s, bias_s, 0, HEAD, slice(None)).astype(bf16)
    keys_head = s_conv[0:HEAD, :NSTATE]
    for (start, width), (out, got, *_) in zip(columns, part_refs):
        for i in range(start // LANES, (start + width) // LANES):
            c = slice(i * LANES, (i + 1) * LANES)
            at = slice(i * LANES - start, (i + 1) * LANES - start)
            x_head = conv_rows(
                x_pad, taps_x[:, c], bias_x[i : i + 1], 0, HEAD, c
            ).astype(bf16)
            x_conv[0:HEAD, c] = x_head
            scaled = (
                x_head.astype(f32) * spread_heads(towards[0:HEAD], spread[:, c])
            ).astype(bf16)
            out[:, at] = (
                main[:, c]
                + lax.dot_general(
                    keys_head, scaled, (((0,), (0,)), ((), ())),
                    preferred_element_type=f32,
                )
            ).astype(bf16)

    def own_rows(j):
        return pl.ds(pl.multiple_of(j * per, per), per)

    for b, (out, got, *_) in enumerate(part_refs):

        def state_start(k, _, b=b, out=out, got=got):
            to = lax.rem(mg + k, g)
            remote(
                out.at[own_rows(to)], got.at[mg], s1_send.at[b], s1_recv.at[b],
                {"seq": base + to},
            ).start()
            return 0

        lax.fori_loop(1, g, state_start, 0)
        got[mg] = out[own_rows(mg)]

    keys = s_conv[:, :NSTATE]
    query = s_conv[:, NSTATE:]
    causal = (
        lax.broadcasted_iota(jnp.int32, (rows, rows), 0)
        >= lax.broadcasted_iota(jnp.int32, (rows, rows), 1)
    )
    scores[...] = jnp.where(
        causal,
        lax.dot_general(
            query, keys, (((1,), (1,)), ((), ())), preferred_element_type=f32
        ),
        0.0,
    )
    first_half = lax.broadcasted_iota(jnp.int32, (1, LANES), 1) < HEAD_DIM
    loads[9].wait()

    def inside(i):
        c = slice(i * LANES, (i + 1) * LANES)
        x_c = x_conv[:, c]
        tops, bottoms = [], []
        for h in (2 * i, 2 * i + 1):
            a_row = shifted[h : h + 1, :]
            top = cols[0:half, h : h + 1] - a_row[:, :half]
            top = scores[0:half, 0:half] * jnp.exp(jnp.minimum(top, 80.0))
            tops.append(
                jnp.dot(top.astype(bf16), x_c[:half], preferred_element_type=f32)
            )
            low = cols[half:, h : h + 1] - a_row
            low = scores[half:, :] * jnp.exp(jnp.minimum(low, 80.0))
            bottoms.append(jnp.dot(low.astype(bf16), x_c, preferred_element_type=f32))
        gain = jnp.where(
            first_half,
            skip_gain[:, 2 * i : 2 * i + 1],
            skip_gain[:, 2 * i + 1 : 2 * i + 2],
        )
        x_f = x_c.astype(f32)
        mixed[0:half, c] = jnp.where(first_half, *tops) + gain * x_f[:half]
        mixed[half:, c] = jnp.where(first_half, *bottoms) + gain * x_f[half:]

    for i in range(tiles):
        inside(i)

    carry_decay = jnp.where(lane == 2, cols[...], 0.0)
    for i in range(tiles):
        c = slice(i * LANES, (i + 1) * LANES)
        decayed[:, c] = spread_heads(carry_decay, spread[:, c])

    wait_for(decay_all.at[pl.ds(0, g - 1)], d_recv)
    decay_cols[...] = spread_heads(
        decay_all[...].reshape(g * 8, LANES), spread[...]
    ).reshape(g, 8, inner)
    loads[10].wait()

    def send_on(b):
        _, _, _, back, ent, passing, coming = part_refs[b]

        @pl.when(me < n - g)
        def _():
            remote(
                passing, coming, c_send.at[b], c_recv.at[b], {"seq": me + g}
            ).start()

        def back_start(k, _):
            to = lax.rem(mg + k, g)

            @pl.when(base + to > 0)
            def _():
                remote(
                    back.at[to], ent.at[own_rows(mg)], s2_send.at[b], s2_recv.at[b],
                    {"seq": base + to},
                ).start()

            return 0

        lax.fori_loop(1, g, back_start, 0)
        ent[own_rows(mg)] = back[mg]

    for b, (start, width) in enumerate(columns):
        _, got, before, back, ent, passing, coming = part_refs[b]
        c = slice(start, start + width)
        wait_for(got.at[pl.ds(0, g - 1)], s1_recv.at[b])
        state = jnp.zeros((per, width), f32)
        for j in range(g):
            before[j] = state
            back[j] = state.astype(bf16)
            state = decay_cols[j][0:1, c] * state + got[j].astype(f32)
        before[g] = state
        passing[...] = state.astype(bf16)

        @pl.when(base == 0)
        def _(b=b):
            send_on(b)

        if b == 0:

            @pl.when(base > 0)
            def _():
                reached = jnp.ones((8, inner), f32)
                for j in range(g):
                    reach[j] = reached
                    reached = reached * decay_cols[j]
                reach[g] = reached

    @pl.when(base > 0)
    def _():
        for b, (start, width) in enumerate(columns):
            _, got, before, back, ent, passing, coming = part_refs[b]
            c = slice(start, start + width)
            remote(
                passing, coming, c_send.at[b], c_recv.at[b], {"seq": me - g}
            ).wait_recv()
            entered = coming[...].astype(f32)
            for j in range(g):
                back[j] = (before[j] + reach[j][0:1, c] * entered).astype(bf16)
            passing[...] = (before[g] + reach[g][0:1, c] * entered).astype(bf16)
            send_on(b)

    @pl.when(me == 0)
    def _():
        ent0[...] = jnp.zeros_like(ent0)
        ent1[...] = jnp.zeros_like(ent1)

    loads[12].wait()

    def across(src, dst, send, recv):
        return remote(src, dst, send, recv, {"tp": other})

    pieces, _, width = part.shape

    def part_copy(p):
        return across(part.at[p], part_got.at[p], o_send.at[p], o_recv.at[p])

    copy_q = across(squares, squares_got, q_sem.at[0], q_sem.at[1])
    total = jnp.zeros((rows, LANES), f32)
    last = len(columns) - 1
    for b, (start, size) in enumerate(columns):
        ent = part_refs[b][4]

        @pl.when(me > 0)
        def _(b=b, ent=ent):
            wait_for(ent.at[pl.ds(0, (g - 1) * per)], s2_recv.at[b])

        for i in range(start // LANES, (start + size) // LANES):
            c = slice(i * LANES, (i + 1) * LANES)
            carried = jnp.dot(
                query, ent[:, i * LANES - start : (i + 1) * LANES - start],
                preferred_element_type=f32,
            )
            raw = (mixed[:, c] + carried * decayed[:, c]) * gate_act[:, c]
            total = total + raw * raw
            gated[:, c] = (raw * norm_gain[i : i + 1]).astype(bf16)
        if b == last:
            squares[...] = total
            copy_q.start()
        c = slice(start, start + size)
        for side in (0, 1):
            owner = other if side == 0 else core
            for p in range(pieces):
                at = pl.ds(pl.multiple_of(owner * inner + p * width, LANES), width)
                value = jnp.dot(
                    gated[:, c], w_all[c, at], preferred_element_type=f32
                )
                if b > 0:
                    value = value + acc[side, p]
                if b == last and side == 0:
                    part[p] = value.astype(bf16)
                    part_copy(p).start()
                else:
                    acc[side, p] = value
    copy_q.wait_recv()
    both = jnp.sum(squares[...] + squares_got[...], axis=1, keepdims=True)
    scale = lax.rsqrt(both / (2 * inner) + 1e-05)
    for p in range(pieces):
        part_copy(p).wait_recv()
        out_ref[:, p * width : (p + 1) * width] = (
            (acc[1, p] + part_got[p].astype(f32)) * scale
        ).astype(bf16)

    copy_q.wait_send()
    for p in range(pieces):
        part_copy(p).wait_send()
    wait_for(decay_all.at[pl.ds(0, g - 1)], d_send)

    @pl.when(me < n - 1)
    def _():
        for copy in rim_copies():
            copy.wait_send()

    for b in range(len(columns)):
        out, got, before, back, ent, passing, coming = part_refs[b]
        wait_for(got.at[pl.ds(0, g - 1)], s1_send.at[b])

        @pl.when((base > 0) | (me == 0))
        def _(b=b, back=back):
            wait_for(back.at[pl.ds(0, g - 1)], s2_send.at[b])

        @pl.when((base == 0) & (me > 0))
        def _(b=b, back=back):
            wait_for(back.at[pl.ds(0, g - 2)], s2_send.at[b])

        @pl.when(me < n - g)
        def _(b=b, passing=passing, coming=coming):
            remote(
                passing, coming, c_send.at[b], c_recv.at[b], {"seq": me + g}
            ).wait_send()


def local(
    inner_input, gate_input, state_input, step_raw, conv_inner, conv_state,
    bias_inner, bias_state, step_bias, decay_log, skip_gain, norm_gain, out_weight,
):
    n = lax.axis_size("seq")
    g = math.gcd(n, 8)
    per = NSTATE // g
    rows, inner = inner_input.shape
    maps = state_input.shape[1]
    width = 256
    pieces = inner // width
    (_, w0), (_, w1) = split_columns(inner)
    vm = pltpu.VMEM
    dma = pltpu.SemaphoreType.DMA
    row = lambda v: v.reshape(1, -1)
    tile = lambda v: v.reshape(-1, LANES)
    operands = (
        inner_input, gate_input, state_input, step_raw, conv_inner, conv_state,
        tile(bias_inner), row(bias_state), row(step_bias), row(decay_log),
        row(skip_gain), tile(norm_gain), out_weight,
    )
    scratch = [vm(v.shape, v.dtype) for v in operands]
    scratch += [
        vm((rows + RIM, inner), f32),
        vm((rows + RIM, maps), f32),
        vm((rows, inner), bf16),
        vm((rows, maps), bf16),
        vm((LANES, rows), f32),
        vm((LANES, inner), bf16),
        vm((rows, LANES), f32),
        vm((rows, rows), f32),
        vm((rows, inner), f32),
        vm((rows, inner), f32),
        vm((rows, inner), f32),
        vm((rows, inner), bf16),
        vm((NSTATE, inner), f32),
        vm((RIM, inner), bf16),
        vm((RIM, maps), bf16),
        vm((8, LANES), f32),
        vm((g, 8, LANES), f32),
        vm((g, 8, inner), f32),
        vm((g + 1, 8, inner), f32),
    ]
    for shape, dtype in (
        ((NSTATE,), bf16), ((g, per), bf16), ((g + 1, per), f32), ((g, per), bf16),
        ((NSTATE,), bf16), ((per,), bf16), ((per,), bf16),
    ):
        scratch += [vm((*shape, w0), dtype), vm((*shape, w1), dtype)]
    scratch += [
        vm((2, pieces, rows, width), f32),
        vm((pieces, rows, width), bf16),
        vm((pieces, rows, width), bf16),
        vm((rows, LANES), f32),
        vm((rows, LANES), f32),
        dma((len(operands),)), dma((2,)), dma((2,)), dma, dma,
        dma((2,)), dma((2,)), dma((2,)), dma((2,)), dma((2,)), dma((2,)),
        dma((pieces,)), dma((pieces,)), dma((2,)),
    ]
    return pl.pallas_call(
        functools.partial(kernel, n, g),
        out_shape=pltpu.VMEM((rows, inner), bf16),
        in_specs=[pl.BlockSpec(memory_space=pltpu.HBM)] * len(operands),
        out_specs=pl.BlockSpec(memory_space=pltpu.VMEM),
        scratch_shapes=scratch,
        compiler_params=pltpu.CompilerParams(
            collective_id=0, has_side_effects=True, vmem_limit_bytes=58 * 2**20
        ),
        name="ssd_block",
    )(*operands)


def solution(mesh):
    return jax.shard_map(
        local,
        mesh=mesh,
        in_specs=(
            P("seq", "tp"),
            P("seq", "tp"),
            P("seq", None),
            P("tp", "seq"),
            P(None, "tp"),
            P(),
            P("tp"),
            P(),
            P("tp"),
            P("tp"),
            P("tp"),
            P("tp"),
            P("tp", None),
        ),
        out_specs=P("seq", "tp"),
        check_vma=False,
    )
```
